32 devices in a mesh: region: 2 (over x), leaf: 16 (over z, y, core).
Axes of the slice: x: 2, y: 2, z: 4, core: 2. Of those that a mesh axis runs over, the one named last changes fastest.
Arguments:
- whiten: bfloat16 [32, 1024, 1024], P(('region', 'leaf')), as said below
- leaf_root: bfloat16 [32, 1024, 512], P(('region', 'leaf')), may hold values from -6 to 6
- leaf_region: bfloat16 [32, 1024, 512], P(('region', 'leaf')), may hold values from -6 to 6
- root_factor: bfloat16 [512, 512], P('region'), may hold values from -0.25 to 0.25
- root_adjoint: bfloat16 [512, 512], P('region'), may hold values from -0.25 to 0.25
- region_factor: bfloat16 [2, 512, 512], P('region', 'leaf'), may hold values from -0.25 to 0.25
- region_adjoint: bfloat16 [2, 512, 512], P('region', 'leaf'), may hold values from -0.25 to 0.25
Outputs:
- grad_root_basis: bfloat16 [32, 1024, 512], P(('region', 'leaf'))
- grad_region_basis: bfloat16 [32, 1024, 512], P(('region', 'leaf'))
- grad_root_factor: float32 [512, 512], P('leaf')
- grad_region_factor: float32 [2, 512, 512], P('region', 'leaf')
The draws below stay inside these ranges and needn't reach their ends.
Inputs may be any that keep to these rules, and one draw needn't show every extreme that they name: `whiten`: each whitening matrix is lower triangular with a positive diagonal.
All inputs are finite; a program needn't handle non-finite values.
Results may differ from the reference program's by a relative error of at most 0.018.
Values may be sent and summed in bfloat16 or wider, within the bound.
A program may use at most 64 MiB of HBM per device.

```python
import jax
import jax.numpy as jnp
from jax import lax

R = 512
M = 512
OBS = 1024
LEAVES = 32
REGIONS = 2


def draw_whiten(key, part):
    first, second = jax.random.split(jax.random.fold_in(key, 17))
    spread = 0.5 * jax.random.normal(first, (LEAVES, OBS, OBS), jnp.float32) / jnp.sqrt(OBS * 1.0)
    lower = jnp.tril(spread, -1)
    diag_vals = jnp.exp(jax.random.uniform(second, (LEAVES, OBS), jnp.float32, jnp.log(0.5), jnp.log(2.0)))
    eye_mat = jnp.eye(OBS, dtype=jnp.float32)
    return (lower + diag_vals[:, :, None] * eye_mat[None]).astype(jnp.bfloat16)


def block_levels(key, extent, shards, least, high):
    level, own = 1.0, jax.random.fold_in(key, 6)
    for position, blocks in shards:
        heights = jnp.exp(jax.random.uniform(jax.random.fold_in(own, position), (blocks,), jnp.float32, least / len(shards), high / len(shards)))
        level = level * jnp.repeat(heights, extent[position] // blocks).reshape([-1 if axis == position else 1 for axis in range(len(extent))])
    return level


def centred(own_key, extent, deviation, bound, cuts=(), held_as=jnp.bfloat16):
    array = deviation * jax.random.normal(own_key, extent, jnp.float32)
    if cuts:
        array = array * block_levels(own_key, extent, cuts, -0.22, 0.18)
    return jnp.clip(array, -bound, bound).astype(held_as)


def setup_inputs(seed: int = 0) -> dict:
    keys = jax.random.split(jax.random.key(seed), 8)
    return {
        "whiten": draw_whiten(jax.random.fold_in(keys[7], 71), 0),
        "leaf_root": centred(keys[1], (LEAVES, OBS, R), 1.0, 6.0, ((0, 32),)),
        "leaf_region": centred(keys[2], (LEAVES, OBS, M), 1.0, 6.0, ((0, 32),)),
        "root_factor": centred(keys[3], (R, R), R ** -0.5, 0.25, ((0, 2),)),
        "root_adjoint": centred(keys[4], (R, R), R ** -0.5, 0.25, ((0, 2),)),
        "region_factor": centred(keys[5], (REGIONS, M, M), M ** -0.5, 0.25, ((0, 2), (1, 16))),
        "region_adjoint": centred(keys[6], (REGIONS, M, M), M ** -0.5, 0.25, ((0, 2), (1, 16))),
    }


def matmul(left, right):
    return jnp.dot(left.astype(jnp.float32), right.astype(jnp.float32), preferred_element_type=jnp.float32)


def reference(whiten, leaf_root, leaf_region, root_factor, root_adjoint, region_factor, region_adjoint):
    root_wide = root_adjoint.astype(jnp.float32)
    region_wide = region_adjoint.astype(jnp.float32)
    root_sym = (root_wide + root_wide.T).astype(jnp.bfloat16)
    region_sym = (region_wide + jnp.swapaxes(region_wide, 1, 2)).astype(jnp.bfloat16)
    per_region = LEAVES // REGIONS

    def visit(carry, inputs):
        root_total, region_total = carry
        factor_inv, base_root, base_region, number = inputs
        owner = (number // per_region).astype(jnp.int32)
        own_factor = lax.dynamic_index_in_dim(region_factor, owner, 0, keepdims=False)
        own_sym = lax.dynamic_index_in_dim(region_sym, owner, 0, keepdims=False)
        root_basis = matmul(base_root, root_factor).astype(jnp.bfloat16)
        region_basis = matmul(base_region, own_factor).astype(jnp.bfloat16)
        root_white = matmul(factor_inv, root_basis).astype(jnp.bfloat16)
        region_white = matmul(factor_inv, region_basis).astype(jnp.bfloat16)
        root_dwhite = matmul(root_white, root_sym).astype(jnp.bfloat16)
        region_dwhite = matmul(region_white, own_sym).astype(jnp.bfloat16)
        grad_root = matmul(factor_inv.T, root_dwhite).astype(jnp.bfloat16)
        grad_region = matmul(factor_inv.T, region_dwhite).astype(jnp.bfloat16)
        root_total = root_total + matmul(base_root.T, grad_root) / OBS
        region_term = matmul(base_region.T, grad_region) / OBS
        old = lax.dynamic_index_in_dim(region_total, owner, 0, keepdims=True)
        region_total = lax.dynamic_update_index_in_dim(region_total, old + region_term[None], owner, 0)
        return (root_total, region_total), (grad_root, grad_region)

    start = (jnp.zeros((R, R), jnp.float32), jnp.zeros((REGIONS, M, M), jnp.float32))
    numbers = jnp.arange(LEAVES, dtype=jnp.int32)
    (root_total, region_total), (grad_root_basis, grad_region_basis) = lax.scan(
        visit, start, (whiten, leaf_root, leaf_region, numbers))
    return grad_root_basis, grad_region_basis, root_total, region_total
```

```python
import functools
import math

import jax
import jax.numpy as jnp
from jax import lax
from jax.experimental import pallas as pl
from jax.experimental.pallas import tpu as pltpu
from jax.sharding import PartitionSpec as P

MESH = pl.DeviceIdType.MESH
F32, BF16 = jnp.float32, jnp.bfloat16


def split_leaf(leaves):
    chips = leaves // 2
    fast = max(d for d in range(1, math.isqrt(chips) + 1) if chips % d == 0)
    return chips // fast, fast


def dot(left, right):
    return jnp.dot(left, right, preferred_element_type=F32)


def kernel(
    nr, nl,
    w_in, lr_in, lg_in, rf_in, ra_in, gf_in, ga_in,
    gr_out, gg_out, fr_out, fg_out,
    w, l, a, b, rt, rg, g, grad, cb, rc, ys, ry, zs, rz, rx,
    ld, st, gz_s, gz_r, gy_s, gy_r, gc_s, gc_r, gx_s, gx_r, gp_s, gp_r,
    cs_s, cs_r, ys_s, ys_r, zs_s, zs_r, xs_s, xs_r,
):
    Z, Y = split_leaf(nl)
    obs, K = l.shape[1], l.shape[2]
    rows, half = K // nl, K // nr
    T = min(256, K)
    nb = obs // T
    r, leaf = lax.axis_index("region"), lax.axis_index("leaf")
    c, y, z = lax.rem(leaf, 2), lax.rem(leaf // 2, Y), leaf // (2 * Y)
    oc = 1 - c

    def at(zz, yy, cc):
        return (zz * Y + yy) * 2 + cc

    def zp(k):
        return lax.rem(z + k, Z)

    def zm(k):
        return lax.rem(z + Z - k, Z)

    def yp(k):
        return lax.rem(y + k, Y)

    def ym(k):
        return lax.rem(y + Y - k, Y)

    def rp(k):
        return lax.rem(r + k, nr)

    def rm(k):
        return lax.rem(r + nr - k, nr)

    def span(index, size):
        return pl.ds(pl.multiple_of(index * size, size), size)

    mine = span(leaf, rows)
    own = span(r, half)
    loads = [
        pltpu.make_async_copy(gf_in.at[0], rg.at[0, mine], ld.at[0]),
        pltpu.make_async_copy(ga_in.at[0], rg.at[1, mine], ld.at[1]),
        pltpu.make_async_copy(rf_in, rt.at[0, own], ld.at[2]),
        pltpu.make_async_copy(ra_in, rt.at[1, own], ld.at[3]),
        pltpu.make_async_copy(lr_in.at[0], l.at[0], ld.at[4]),
        pltpu.make_async_copy(w_in.at[0], w, ld.at[5]),
        pltpu.make_async_copy(lg_in.at[0], l.at[1], ld.at[6]),
    ]
    for load in loads:
        load.start()

    barrier = pltpu.get_barrier_semaphore()
    peers = [{"leaf": at(zp(k), y, c)} for k in range(1, Z)]
    peers += [{"leaf": at(z, yp(k), c)} for k in range(1, Y)]
    peers += [{"leaf": at(z, y, oc)}]
    peers += [{"region": rp(k)} for k in range(1, nr)]
    for peer in peers:
        pl.semaphore_signal(barrier, inc=1, device_id=peer, device_id_type=MESH)
    for load in loads[:4]:
        load.wait()
    pl.semaphore_wait(barrier, len(peers))

    sends = []

    def remote(src, dst, ssem, rsem, peer):
        return pltpu.make_async_remote_copy(
            src_ref=src, dst_ref=dst, send_sem=ssem, recv_sem=rsem,
            device_id=peer, device_id_type=MESH,
        )

    def send(src, dst, ssem, rsem, peer):
        copy = remote(src, dst, ssem, rsem, peer)
        copy.start()
        sends.append(copy)

    def arrive(ref, ssem, rsem, peer):
        remote(ref, ref, ssem, rsem, peer).wait_recv()

    other = {"leaf": at(z, y, oc)}

    def block(kz, ky, cc):
        return rg.at[:, span(at(zm(kz), ym(ky), cc), rows)]

    def gather_y(kz):
        for ky in range(1, Y):
            i = (ky - 1) * Z + kz
            send(block(kz, 0, c), block(kz, 0, c), gy_s.at[i], gy_r.at[i], {"leaf": at(z, yp(ky), c)})

    def gather_core(kz, ky):
        i = ky * Z + kz
        send(block(kz, ky, c), block(kz, ky, c), gc_s.at[i], gc_r.at[i], other)

    def z_forward(kz):
        arrive(block(kz, 0, c), gz_s.at[kz - 1], gz_r.at[kz - 1], other)
        gather_y(kz)
        gather_core(kz, 0)

    def y_forward(kz, ky):
        i = (ky - 1) * Z + kz
        arrive(block(kz, ky, c), gy_s.at[i], gy_r.at[i], other)
        gather_core(kz, ky)

    for k in range(1, Z):
        send(block(0, 0, c), block(0, 0, c), gz_s.at[k - 1], gz_r.at[k - 1], {"leaf": at(zp(k), y, c)})
    gather_y(0)
    for k in range(1, nr):
        send(rt.at[c, own], rt.at[c, own], gx_s.at[k - 1], gx_r.at[k - 1], {"region": rp(k)})
    gather_core(0, 0)

    scale = 1.0 / obs

    def local_a(p):
        for n in range(K // T):
            cols = pl.ds(n * T, T)
            for i in range(nb):
                a[p, pl.ds(i * T, T), cols] = dot(
                    w[pl.ds(i * T, T), pl.ds(0, (i + 1) * T)], l[p, pl.ds(0, (i + 1) * T), cols]
                ).astype(BF16)

    def local_c(p):
        per = T // (2 * Y * rows) if T >= 2 * Y * rows else 0
        step = T if per else 2 * Y * rows
        per = step // (2 * Y * rows)
        for i in range(K // step):
            left = a[p, :, pl.ds(i * step, step)].T
            part = (dot(left, a[p]) * scale).astype(BF16)
            cb[p, pl.ds(i * per, per)] = part.reshape(per, Y, 2, rows, K)
        send(cb.at[p, :, :, oc], rc.at[p], cs_s.at[p], cs_r.at[p], other)

    def local_b(i):
        left = w[pl.ds(i * T, obs - i * T), pl.ds(i * T, T)].T
        for p in range(2):
            b[p, pl.ds(i * T, T), :] = dot(left, a[p, pl.ds(i * T, obs - i * T), :]).astype(BF16)

    def reduce_y(p):
        arrive(rc.at[p], cs_s.at[p], cs_r.at[p], other)
        for k in range(1, Y):
            ys[p, k - 1] = (cb[p, :, yp(k), c].astype(F32) + rc[p, :, yp(k)].astype(F32)).astype(BF16)
            i = p * Y + k
            send(ys.at[p, k - 1], ry.at[p, k - 1], ys_s.at[i], ys_r.at[i], {"leaf": at(z, yp(k), c)})

    def chip_sum(p, zz):
        total = cb[p, zz, y, c].astype(F32) + rc[p, zz, y].astype(F32)
        for k in range(1, Y):
            total += ry[p, k - 1, zz].astype(F32)
        return total

    def reduce_z(p):
        for k in range(1, Y):
            i = p * Y + k
            arrive(ry.at[p, k - 1], ys_s.at[i], ys_r.at[i], other)
        for k in range(1, Z):
            zs[p, k - 1] = chip_sum(p, zp(k)).astype(BF16)
            i = p * Z + k
            send(zs.at[p, k - 1], rz.at[p, k - 1], zs_s.at[i], zs_r.at[i], {"leaf": at(zp(k), y, c)})

    def finish_z(p):
        total = chip_sum(p, z)
        for k in range(1, Z):
            i = p * Z + k
            arrive(rz.at[p, k - 1], zs_s.at[i], zs_r.at[i], other)
            total += rz[p, k - 1].astype(F32)
        return total

    def make_g(p, held):
        factor, adjoint = held[0], held[1]
        both = dot(factor, adjoint) + lax.dot_general(
            factor, adjoint, (((1,), (1,)), ((), ())), preferred_element_type=F32
        )
        g[p] = both.astype(BF16)

    def make_grad(p, out):
        for i in range(nb):
            grad[p, pl.ds(i * T, T), :] = dot(b[p, pl.ds(i * T, T), :], g[p]).astype(BF16)
        copy = pltpu.make_async_copy(grad.at[p], out.at[0], st.at[p])
        copy.start()
        return copy

    loads[4].wait()
    loads[5].wait()
    local_a(0)
    local_c(0)
    loads[6].wait()
    local_a(1)
    local_c(1)
    local_b(0)
    reduce_y(0)
    if Z > 1:
        z_forward(1)
    local_b(1)
    reduce_y(1)
    for k in range(2, Z):
        z_forward(k)
    for i in range(2, nb):
        local_b(i)
    for ky in range(1, Y):
        y_forward(0, ky)
    for k in range(1, nr):
        theirs = rt.at[c, span(rm(k), half)]
        arrive(theirs, gx_s.at[k - 1], gx_r.at[k - 1], other)
        send(theirs, theirs, gp_s.at[k - 1], gp_r.at[k - 1], other)
    reduce_z(0)
    for ky in range(1, Y):
        for k in range(1, Z):
            y_forward(k, ky)
    for k in range(1, nr):
        arrive(rt.at[oc, span(rm(k), half)], gp_s.at[k - 1], gp_r.at[k - 1], other)
    make_g(0, rt)
    store_root = make_grad(0, gr_out)
    reduce_z(1)
    rx[r] = finish_z(0).astype(BF16)
    for k in range(1, nr):
        send(rx.at[r], rx.at[r], xs_s.at[k - 1], xs_r.at[k - 1], {"region": rp(k)})
    for ky in range(Y):
        for kz in range(Z):
            i = ky * Z + kz
            arrive(block(kz, ky, oc), gc_s.at[i], gc_r.at[i], other)
    make_g(1, rg)
    store_region = make_grad(1, gg_out)
    fg_out[0] = dot(finish_z(1).astype(BF16), g[1])
    for k in range(1, nr):
        arrive(rx.at[rm(k)], xs_s.at[k - 1], xs_r.at[k - 1], other)
    total = rx[0].astype(F32)
    for k in range(1, nr):
        total += rx[k].astype(F32)
    fr_out[...] = dot(total.astype(BF16), g[0])
    store_root.wait()
    store_region.wait()
    for copy in sends:
        copy.wait_send()


def solution(mesh):
    nr, nl = mesh.shape["region"], mesh.shape["leaf"]
    Z, Y = split_leaf(nl)

    def on_device(whiten, leaf_root, leaf_region, root_factor, root_adjoint, region_factor, region_adjoint):
        obs, K = leaf_root.shape[1], leaf_root.shape[2]
        rows = K // nl
        dma = lambda n: pltpu.SemaphoreType.DMA((max(n, 1),))
        return pl.pallas_call(
            functools.partial(kernel, nr, nl),
            out_shape=(
                jax.ShapeDtypeStruct(leaf_root.shape, BF16),
                jax.ShapeDtypeStruct(leaf_region.shape, BF16),
                jax.ShapeDtypeStruct((rows, K), F32),
                jax.ShapeDtypeStruct((1, rows, K), F32),
            ),
            in_specs=[pl.BlockSpec(memory_space=pl.ANY)] * 7,
            out_specs=(
                pl.BlockSpec(memory_space=pl.ANY),
                pl.BlockSpec(memory_space=pl.ANY),
                pl.BlockSpec(memory_space=pltpu.VMEM),
                pl.BlockSpec(memory_space=pltpu.VMEM),
            ),
            scratch_shapes=[
                pltpu.VMEM((obs, obs), BF16),
                pltpu.VMEM((2, obs, K), BF16),
                pltpu.VMEM((2, obs, K), BF16),
                pltpu.VMEM((2, obs, K), BF16),
                pltpu.VMEM((2, K, K), BF16),
                pltpu.VMEM((2, K, K), BF16),
                pltpu.VMEM((2, K, K), BF16),
                pltpu.VMEM((2, obs, K), BF16),
                pltpu.VMEM((2, Z, Y, 2, rows, K), BF16),
                pltpu.VMEM((2, Z, Y, rows, K), BF16),
                pltpu.VMEM((2, max(Y - 1, 1), Z, rows, K), BF16),
                pltpu.VMEM((2, max(Y - 1, 1), Z, rows, K), BF16),
                pltpu.VMEM((2, max(Z - 1, 1), rows, K), BF16),
                pltpu.VMEM((2, max(Z - 1, 1), rows, K), BF16),
                pltpu.VMEM((nr, rows, K), BF16),
                dma(7), dma(2),
                dma(Z - 1), dma(Z - 1),
                dma((Y - 1) * Z), dma((Y - 1) * Z),
                dma(Y * Z), dma(Y * Z),
                dma(nr - 1), dma(nr - 1),
                dma(nr - 1), dma(nr - 1),
                dma(2), dma(2),
                dma(2 * Y), dma(2 * Y),
                dma(2 * Z), dma(2 * Z),
                dma(nr - 1), dma(nr - 1),
            ],
            compiler_params=pltpu.CompilerParams(
                collective_id=0, has_side_effects=True, vmem_limit_bytes=48 * 1024 * 1024
            ),
            name="likelihood_backward",
        )(whiten, leaf_root, leaf_region, root_factor, root_adjoint, region_factor, region_adjoint)

    return jax.shard_map(
        on_device,
        mesh=mesh,
        in_specs=(
            P(("region", "leaf"), None, None),
            P(("region", "leaf"), None, None),
            P(("region", "leaf"), None, None),
            P("region", None),
            P("region", None),
            P("region", "leaf", None),
            P("region", "leaf", None),
        ),
        out_specs=(
            P(("region", "leaf"), None, None),
            P(("region", "leaf"), None, None),
            P("leaf", None),
            P("region", "leaf", None),
        ),
        check_vma=False,
    )
```

```python
import functools
import math

import jax
import jax.numpy as jnp
from jax import lax
from jax.experimental import pallas as pl
from jax.experimental.pallas import tpu as pltpu
from jax.sharding import PartitionSpec as P

MESH = pl.DeviceIdType.MESH
F32, BF16 = jnp.float32, jnp.bfloat16


def split_leaf(leaves):
    chips = leaves // 2
    fast = max(d for d in range(1, math.isqrt(chips) + 1) if chips % d == 0)
    return chips // fast, fast


def offset(value, step, count):
    if count & (count - 1):
        return lax.rem(value + step, count), lax.rem(value + count - step, count)
    bit = 1
    pair = value
    while bit < count:
        if step & bit:
            pair = pair + bit - 2 * bit * lax.rem(value // bit, 2)
        bit *= 2
    return pair, pair


def dot(left, right):
    return jnp.dot(left, right, preferred_element_type=F32)


def kernel(
    nr, nl,
    w_in, lr_in, lg_in, rf_in, ra_in, gf_in, ga_in,
    gr_out, gg_out, fr_out, fg_out,
    w, l, a, b, rt, rg, g, grad, cb, rc, ys, ry, zs, rz, rx,
    ld, st, gz_s, gz_r, gy_s, gy_r, gc_s, gc_r, gx_s, gx_r, gp_s, gp_r,
    cs_s, cs_r, ys_s, ys_r, zs_s, zs_r, xs_s, xs_r,
):
    Z, Y = split_leaf(nl)
    obs, K = l.shape[1], l.shape[2]
    rows, half = K // nl, K // nr
    T = min(256, K)
    nb = obs // T
    r, leaf = lax.axis_index("region"), lax.axis_index("leaf")
    c, y, z = lax.rem(leaf, 2), lax.rem(leaf // 2, Y), leaf // (2 * Y)
    oc = 1 - c

    def at(zz, yy, cc):
        return (zz * Y + yy) * 2 + cc

    def zp(k):
        return offset(z, k, Z)[0]

    def zm(k):
        return offset(z, k, Z)[1]

    def yp(k):
        return offset(y, k, Y)[0]

    def ym(k):
        return offset(y, k, Y)[1]

    def rp(k):
        return lax.rem(r + k, nr)

    def rm(k):
        return lax.rem(r + nr - k, nr)

    def span(index, size):
        return pl.ds(pl.multiple_of(index * size, size), size)

    mine = span(leaf, rows)
    own = span(r, half)
    loads = [
        pltpu.make_async_copy(gf_in.at[0], rg.at[0, mine], ld.at[0]),
        pltpu.make_async_copy(ga_in.at[0], rg.at[1, mine], ld.at[1]),
        pltpu.make_async_copy(rf_in, rt.at[0, own], ld.at[2]),
        pltpu.make_async_copy(ra_in, rt.at[1, own], ld.at[3]),
        pltpu.make_async_copy(lr_in.at[0], l.at[0], ld.at[4]),
        pltpu.make_async_copy(w_in.at[0], w, ld.at[5]),
        pltpu.make_async_copy(lg_in.at[0], l.at[1], ld.at[6]),
    ]
    for load in loads:
        load.start()

    barrier = pltpu.get_barrier_semaphore()
    peers = [{"leaf": at(zp(k), y, c)} for k in range(1, Z)]
    peers += [{"leaf": at(z, yp(k), c)} for k in range(1, Y)]
    peers += [{"leaf": at(z, y, oc)}]
    peers += [{"region": rp(k)} for k in range(1, nr)]
    for peer in peers:
        pl.semaphore_signal(barrier, inc=1, device_id=peer, device_id_type=MESH)
    for load in loads[:4]:
        load.wait()
    pl.semaphore_wait(barrier, len(peers))

    sends = []

    def remote(src, dst, ssem, rsem, peer):
        return pltpu.make_async_remote_copy(
            src_ref=src, dst_ref=dst, send_sem=ssem, recv_sem=rsem,
            device_id=peer, device_id_type=MESH,
        )

    def send(src, dst, ssem, rsem, peer):
        copy = remote(src, dst, ssem, rsem, peer)
        copy.start()
        sends.append(copy)

    def arrive(ref, ssem, rsem, peer):
        remote(ref, ref, ssem, rsem, peer).wait_recv()

    other = {"leaf": at(z, y, oc)}

    def block(kz, ky, cc):
        return rg.at[:, span(at(zm(kz), ym(ky), cc), rows)]

    def gather_y(kz):
        for ky in range(1, Y):
            i = (ky - 1) * Z + kz
            send(block(kz, 0, c), block(kz, 0, c), gy_s.at[i], gy_r.at[i], {"leaf": at(z, yp(ky), c)})

    def gather_core(kz, ky):
        i = ky * Z + kz
        send(block(kz, ky, c), block(kz, ky, c), gc_s.at[i], gc_r.at[i], other)

    def z_forward(kz):
        arrive(block(kz, 0, c), gz_s.at[kz - 1], gz_r.at[kz - 1], other)
        gather_y(kz)
        gather_core(kz, 0)

    def y_forward(kz, ky):
        i = (ky - 1) * Z + kz
        arrive(block(kz, ky, c), gy_s.at[i], gy_r.at[i], other)
        gather_core(kz, ky)

    for k in range(1, Z):
        send(block(0, 0, c), block(0, 0, c), gz_s.at[k - 1], gz_r.at[k - 1], {"leaf": at(zp(k), y, c)})
    gather_y(0)
    for k in range(1, nr):
        send(rt.at[c, own], rt.at[c, own], gx_s.at[k - 1], gx_r.at[k - 1], {"region": rp(k)})
    gather_core(0, 0)

    scale = 1.0 / obs

    def local_a(p):
        for n in range(K // T):
            cols = pl.ds(n * T, T)
            for i in range(nb):
                a[p, pl.ds(i * T, T), cols] = dot(
                    w[pl.ds(i * T, T), pl.ds(0, (i + 1) * T)], l[p, pl.ds(0, (i + 1) * T), cols]
                ).astype(BF16)

    def local_c(p):
        per = T // (2 * Y * rows) if T >= 2 * Y * rows else 0
        step = T if per else 2 * Y * rows
        per = step // (2 * Y * rows)
        for i in range(K // step):
            left = a[p, :, pl.ds(i * step, step)].T
            part = (dot(left, a[p]) * scale).astype(BF16)
            cb[p, pl.ds(i * per, per)] = part.reshape(per, Y, 2, rows, K)
        send(cb.at[p, :, :, oc], rc.at[p], cs_s.at[p], cs_r.at[p], other)

    def local_b(i):
        left = w[pl.ds(i * T, obs - i * T), pl.ds(i * T, T)].T
        for p in range(2):
            b[p, pl.ds(i * T, T), :] = dot(left, a[p, pl.ds(i * T, obs - i * T), :]).astype(BF16)

    far = range(Z - 1, -1, -1)

    def reduce_y(p):
        arrive(rc.at[p], cs_s.at[p], cs_r.at[p], other)
        for kz in far:
            zz = zp(kz)
            for k in range(1, Y):
                yy = yp(k)
                ys[p, k - 1, kz] = (cb[p, zz, yy, c].astype(F32) + rc[p, zz, yy].astype(F32)).astype(BF16)
                i = (p * Y + k) * Z + kz
                send(ys.at[p, k - 1, kz], ry.at[p, k - 1, kz], ys_s.at[i], ys_r.at[i], {"leaf": at(z, yy, c)})

    def chip_sum(p, kz):
        zz = zp(kz)
        total = cb[p, zz, y, c].astype(F32) + rc[p, zz, y].astype(F32)
        for k in range(1, Y):
            i = (p * Y + k) * Z + kz
            arrive(ry.at[p, k - 1, kz], ys_s.at[i], ys_r.at[i], other)
            total += ry[p, k - 1, kz].astype(F32)
        return total

    def reduce_z(p):
        for k in far[:-1]:
            zs[p, k - 1] = chip_sum(p, k).astype(BF16)
            i = p * Z + k
            send(zs.at[p, k - 1], rz.at[p, k - 1], zs_s.at[i], zs_r.at[i], {"leaf": at(zp(k), y, c)})

    def finish_z(p):
        total = chip_sum(p, 0)
        for k in range(1, Z):
            i = p * Z + k
            arrive(rz.at[p, k - 1], zs_s.at[i], zs_r.at[i], other)
            total += rz[p, k - 1].astype(F32)
        return total

    def make_g(p, held):
        factor, adjoint = held[0], held[1]
        both = dot(factor, adjoint) + lax.dot_general(
            factor, adjoint, (((1,), (1,)), ((), ())), preferred_element_type=F32
        )
        g[p] = both.astype(BF16)

    def make_grad(p, out):
        for i in range(nb):
            part = pl.ds(i * T, T)
            grad[p, part, :] = dot(b[p, part, :], g[p]).astype(BF16)
        copy = pltpu.make_async_copy(grad.at[p], out.at[0], st.at[p])
        copy.start()
        return copy

    loads[4].wait()
    loads[5].wait()
    local_a(0)
    local_c(0)
    if Z > 1:
        z_forward(1)
    loads[6].wait()
    local_a(1)
    local_c(1)
    if Z > 2:
        z_forward(2)
    local_b(0)
    reduce_y(0)
    for k in range(3, Z):
        z_forward(k)
    reduce_y(1)
    for i in range(1, nb):
        local_b(i)
    for ky in range(1, Y):
        y_forward(0, ky)
    reduce_z(0)
    for k in range(1, nr):
        theirs = rt.at[c, span(rm(k), half)]
        arrive(theirs, gx_s.at[k - 1], gx_r.at[k - 1], other)
        send(theirs, theirs, gp_s.at[k - 1], gp_r.at[k - 1], other)
    for ky in range(1, Y):
        for k in range(1, Z):
            y_forward(k, ky)
    reduce_z(1)
    for k in range(1, nr):
        arrive(rt.at[oc, span(rm(k), half)], gp_s.at[k - 1], gp_r.at[k - 1], other)
    make_g(0, rt)
    rx[r] = finish_z(0).astype(BF16)
    for k in range(1, nr):
        send(rx.at[r], rx.at[r], xs_s.at[k - 1], xs_r.at[k - 1], {"region": rp(k)})
    stores = [make_grad(0, gr_out)]
    for ky in range(Y):
        for kz in range(Z):
            i = ky * Z + kz
            arrive(block(kz, ky, oc), gc_s.at[i], gc_r.at[i], other)
    make_g(1, rg)
    stores.append(make_grad(1, gg_out))
    fg_out[0] = dot(finish_z(1).astype(BF16), g[1])
    for k in range(1, nr):
        arrive(rx.at[rm(k)], xs_s.at[k - 1], xs_r.at[k - 1], other)
    total = rx[0].astype(F32)
    for k in range(1, nr):
        total += rx[k].astype(F32)
    fr_out[...] = dot(total.astype(BF16), g[0])
    for copy in stores:
        copy.wait()
    for copy in sends:
        copy.wait_send()


def store(*refs):
    source, target, held = refs[:4], refs[4:8], refs[8:12]
    load_sem, store_sem = refs[12:]
    pieces = []
    for n in range(4):
        extent = source[n].shape[-2]
        size = min(extent, 256)
        for row in range(0, extent, size):
            where = (pl.ds(row, size),) if len(source[n].shape) == 2 else (0, pl.ds(row, size))
            pieces.append((source[n].at[where], held[n].at[where], target[n].at[where]))
    loads = [pltpu.make_async_copy(p[0], p[1], load_sem.at[i]) for i, p in enumerate(pieces)]
    stores = [pltpu.make_async_copy(p[1], p[2], store_sem.at[i]) for i, p in enumerate(pieces)]
    for load in loads:
        load.start()
    for load, save in zip(loads, stores):
        load.wait()
        save.start()
    for save in stores:
        save.wait()


def solution(mesh):
    nr, nl = mesh.shape["region"], mesh.shape["leaf"]
    Z, Y = split_leaf(nl)

    def on_device(whiten, leaf_root, leaf_region, root_factor, root_adjoint, region_factor, region_adjoint):
        obs, K = leaf_root.shape[1], leaf_root.shape[2]
        rows = K // nl
        dma = lambda n: pltpu.SemaphoreType.DMA((max(n, 1),))
        held = pl.pallas_call(
            functools.partial(kernel, nr, nl),
            out_shape=(
                jax.ShapeDtypeStruct(leaf_root.shape, BF16),
                jax.ShapeDtypeStruct(leaf_region.shape, BF16),
                jax.ShapeDtypeStruct((rows, K), F32),
                jax.ShapeDtypeStruct((1, rows, K), F32),
            ),
            in_specs=[pl.BlockSpec(memory_space=pltpu.HBM)] * 7,
            out_specs=(pl.BlockSpec(memory_space=pltpu.HBM),) * 2 + (pl.BlockSpec(memory_space=pltpu.VMEM),) * 2,
            scratch_shapes=[
                pltpu.VMEM((obs, obs), BF16),
                pltpu.VMEM((2, obs, K), BF16),
                pltpu.VMEM((2, obs, K), BF16),
                pltpu.VMEM((2, obs, K), BF16),
                pltpu.VMEM((2, K, K), BF16),
                pltpu.VMEM((2, K, K), BF16),
                pltpu.VMEM((2, K, K), BF16),
                pltpu.VMEM((2, obs, K), BF16),
                pltpu.VMEM((2, Z, Y, 2, rows, K), BF16),
                pltpu.VMEM((2, Z, Y, rows, K), BF16),
                pltpu.VMEM((2, max(Y - 1, 1), Z, rows, K), BF16),
                pltpu.VMEM((2, max(Y - 1, 1), Z, rows, K), BF16),
                pltpu.VMEM((2, max(Z - 1, 1), rows, K), BF16),
                pltpu.VMEM((2, max(Z - 1, 1), rows, K), BF16),
                pltpu.VMEM((nr, rows, K), BF16),
                dma(7), dma(2),
                dma(Z - 1), dma(Z - 1),
                dma((Y - 1) * Z), dma((Y - 1) * Z),
                dma(Y * Z), dma(Y * Z),
                dma(nr - 1), dma(nr - 1),
                dma(nr - 1), dma(nr - 1),
                dma(2), dma(2),
                dma(2 * Y * Z), dma(2 * Y * Z),
                dma(2 * Z), dma(2 * Z),
                dma(nr - 1), dma(nr - 1),
            ],
            compiler_params=pltpu.CompilerParams(
                collective_id=0, has_side_effects=True, vmem_limit_bytes=67043328
            ),
            name="likelihood_backward",
        )(whiten, leaf_root, leaf_region, root_factor, root_adjoint, region_factor, region_adjoint)
        return pl.pallas_call(
            store,
            out_shape=tuple(jax.ShapeDtypeStruct(x.shape, x.dtype) for x in held),
            in_specs=[pl.BlockSpec(memory_space=pltpu.HBM)] * 4,
            out_specs=(pl.BlockSpec(memory_space=pltpu.HBM),) * 4,
            scratch_shapes=[pltpu.VMEM(x.shape, x.dtype) for x in held] + [dma(2 * pl.cdiv(obs, 256) + 2)] * 2,
            compiler_params=pltpu.CompilerParams(vmem_limit_bytes=67043328),
            name="store_outputs",
        )(*held)

    return jax.shard_map(
        on_device,
        mesh=mesh,
        in_specs=(
            P(("region", "leaf"), None, None),
            P(("region", "leaf"), None, None),
            P(("region", "leaf"), None, None),
            P("region", None),
            P("region", None),
            P("region", "leaf", None),
            P("region", "leaf", None),
        ),
        out_specs=(
            P(("region", "leaf"), None, None),
            P(("region", "leaf"), None, None),
            P("leaf", None),
            P("region", "leaf", None),
        ),
        check_vma=False,
    )
```
